32 devices in a mesh: tp: 4 (over z), ep: 8 (over y, x, core).
Axes of the slice: x: 2, y: 2, z: 4, core: 2. Of those that a mesh axis runs over, the one named last changes fastest.
Arguments:
- hidden_in: bfloat16 [1024, 2048], P(('tp', 'ep'))
- cache0: bfloat16 [1024, 256, 576], P(('tp', 'ep'))
- cache1: bfloat16 [1024, 256, 576], P(('tp', 'ep'))
- kv_lens: int32 [1024], P(('tp', 'ep'))
- route_ids: int32 [1024, 6], P(('tp', 'ep'))
- route_wts: float32 [1024, 6], P(('tp', 'ep'))
- att0_q: bfloat16 [2048, 16, 192], replicated
- att0_uk: bfloat16 [16, 128, 512], replicated
- att0_uv: bfloat16 [16, 512, 128], replicated
- att0_o: bfloat16 [16, 128, 2048], replicated
- att1_q: bfloat16 [2048, 16, 192], replicated
- att1_uk: bfloat16 [16, 128, 512], replicated
- att1_uv: bfloat16 [16, 512, 128], replicated
- att1_o: bfloat16 [16, 128, 2048], replicated
- ffn0_gate: bfloat16 [2048, 10944], P(None, 'tp')
- ffn0_up: bfloat16 [2048, 10944], P(None, 'tp')
- ffn0_down: bfloat16 [10944, 2048], P('tp')
- ffn1_gate: bfloat16 [2048, 10944], P(None, 'tp')
- ffn1_up: bfloat16 [2048, 10944], P(None, 'tp')
- ffn1_down: bfloat16 [10944, 2048], P('tp')
- exp_gate: bfloat16 [32, 2048, 1408], P(('tp', 'ep'))
- exp_up: bfloat16 [32, 2048, 1408], P(('tp', 'ep'))
- exp_down: bfloat16 [32, 1408, 2048], P(('tp', 'ep'))
Outputs:
- output: bfloat16 [1024, 2048], P(('tp', 'ep'))
All inputs are finite; a program needn't handle non-finite values.
Results may differ from the reference program's by a relative error of at most 0.015514.
Values are sent between devices in bfloat16 or wider.
A program may use at most 1 GiB of HBM per device.

```python
import jax
import jax.numpy as jnp
from jax import lax

HIDDEN = 2048
NUM_HEADS = 16
NOPE_DIM = 128
ROPE_DIM = 64
VALUE_DIM = 128
LATENT = 512
TOP_K = 6
FF_EXPERT = 1408
FF_DENSE = 10944
TOK_DEV = 32
KV_LEN = 256
ZERO_EXPERTS = 24
DEVICES = 32

NUM_TOKENS = TOK_DEV * DEVICES
SLOT_CAP = min(TOK_DEV, (2 * TOK_DEV * TOP_K + DEVICES - 1) // DEVICES)
ROWS_MAX = DEVICES * SLOT_CAP
NUM_HOT = max(1, DEVICES // 16)
COLD_SLOTS = (TOK_DEV * TOP_K * 3) // 5 - NUM_HOT * SLOT_CAP
SCALE = (NOPE_DIM + ROPE_DIM) ** -0.5


def draw_normal(key, shape, scale):
    return (jax.random.normal(key, shape, jnp.float32) * scale).astype(jnp.bfloat16)


def draw_routes(key):
    key_hot, key_src = jax.random.split(key)
    dev_order = jax.random.permutation(key_hot, DEVICES)
    hot_flag = jnp.zeros((DEVICES,), jnp.int32).at[dev_order[:NUM_HOT]].set(1)
    cold_devs = dev_order[NUM_HOT:]

    def one_source(src):
        src_key = jax.random.fold_in(key_src, src)
        key_pick, key_zero, key_perm = jax.random.split(src_key, 3)
        cold_pick = cold_devs[jax.random.randint(key_pick, (COLD_SLOTS,), 0, DEVICES - NUM_HOT)]
        dev_counts = jax.ops.segment_sum(jnp.ones((COLD_SLOTS,), jnp.int32), cold_pick, num_segments=DEVICES)
        dev_counts = jnp.where(hot_flag == 1, SLOT_CAP, jnp.minimum(dev_counts, SLOT_CAP))
        dev_bounds = jnp.cumsum(dev_counts)
        dest_dev = jnp.searchsorted(dev_bounds, jnp.arange(TOK_DEV * TOP_K), side='right').astype(jnp.int32)
        dest_dev = dest_dev.reshape(TOP_K, TOK_DEV).T
        zero_base = jax.random.randint(key_zero, (TOK_DEV, 1), 0, ZERO_EXPERTS)
        zero_ids = DEVICES + (jnp.arange(TOP_K)[None, :] + zero_base) % ZERO_EXPERTS
        slot_ids = jnp.where(dest_dev < DEVICES, dest_dev, zero_ids).astype(jnp.int32)
        return slot_ids[jax.random.permutation(key_perm, TOK_DEV)]

    return jax.vmap(one_source)(jnp.arange(DEVICES)).reshape(NUM_TOKENS, TOP_K)


def draw_lengths(key):
    lengths = jax.random.randint(key, (NUM_TOKENS,), KV_LEN // 8, KV_LEN + 1)
    return lengths.at[0].set(KV_LEN).astype(jnp.int32)


def setup_inputs(seed: int = 0) -> dict:
    keys = jax.random.split(jax.random.key(seed), 26)
    qk_dim = NOPE_DIM + ROPE_DIM
    uv_scale = LATENT ** -0.5 * KV_LEN ** 0.5 / 4.0
    return {
        'hidden_in': draw_normal(keys[0], (NUM_TOKENS, HIDDEN), 1.0),
        'cache0': draw_normal(keys[1], (NUM_TOKENS, KV_LEN, LATENT + ROPE_DIM), 1.0),
        'cache1': draw_normal(keys[2], (NUM_TOKENS, KV_LEN, LATENT + ROPE_DIM), 1.0),
        'kv_lens': draw_lengths(keys[3]),
        'route_ids': draw_routes(keys[4]),
        'route_wts': jax.random.uniform(keys[5], (NUM_TOKENS, TOP_K), jnp.float32, 0.5, 1.5) * (2.0 / TOP_K),
        'att0_q': draw_normal(keys[6], (HIDDEN, NUM_HEADS, qk_dim), HIDDEN ** -0.5),
        'att0_uk': draw_normal(keys[7], (NUM_HEADS, NOPE_DIM, LATENT), NOPE_DIM ** -0.5),
        'att0_uv': draw_normal(keys[8], (NUM_HEADS, LATENT, VALUE_DIM), uv_scale),
        'att0_o': draw_normal(keys[9], (NUM_HEADS, VALUE_DIM, HIDDEN), (NUM_HEADS * VALUE_DIM) ** -0.5),
        'att1_q': draw_normal(keys[10], (HIDDEN, NUM_HEADS, qk_dim), HIDDEN ** -0.5),
        'att1_uk': draw_normal(keys[11], (NUM_HEADS, NOPE_DIM, LATENT), NOPE_DIM ** -0.5),
        'att1_uv': draw_normal(keys[12], (NUM_HEADS, LATENT, VALUE_DIM), uv_scale),
        'att1_o': draw_normal(keys[13], (NUM_HEADS, VALUE_DIM, HIDDEN), (NUM_HEADS * VALUE_DIM) ** -0.5),
        'ffn0_gate': draw_normal(keys[14], (HIDDEN, FF_DENSE), HIDDEN ** -0.5),
        'ffn0_up': draw_normal(keys[15], (HIDDEN, FF_DENSE), HIDDEN ** -0.5),
        'ffn0_down': draw_normal(keys[16], (FF_DENSE, HIDDEN), FF_DENSE ** -0.5),
        'ffn1_gate': draw_normal(keys[17], (HIDDEN, FF_DENSE), HIDDEN ** -0.5),
        'ffn1_up': draw_normal(keys[18], (HIDDEN, FF_DENSE), HIDDEN ** -0.5),
        'ffn1_down': draw_normal(keys[19], (FF_DENSE, HIDDEN), FF_DENSE ** -0.5),
        'exp_gate': draw_normal(keys[20], (DEVICES, HIDDEN, FF_EXPERT), HIDDEN ** -0.5),
        'exp_up': draw_normal(keys[21], (DEVICES, HIDDEN, FF_EXPERT), HIDDEN ** -0.5),
        'exp_down': draw_normal(keys[22], (DEVICES, FF_EXPERT, HIDDEN), 2.0 * FF_EXPERT ** -0.5),
    }


def rms_norm(vec):
    vec32 = vec.astype(jnp.float32)
    return (vec32 * lax.rsqrt(jnp.mean(vec32 * vec32, axis=-1, keepdims=True) + 1e-6)).astype(jnp.bfloat16)


def rope_rotate(vals, pos):
    half_dim = vals.shape[-1] // 2
    inv_freq = 10000.0 ** (-2.0 * jnp.arange(half_dim, dtype=jnp.float32) / vals.shape[-1])
    rot_angle = pos.astype(jnp.float32)[..., None, None] * inv_freq
    cos_ang = jnp.cos(rot_angle)
    sin_ang = jnp.sin(rot_angle)
    lead_half = vals[..., :half_dim]
    tail_half = vals[..., half_dim:]
    return jnp.concatenate([lead_half * cos_ang - tail_half * sin_ang, tail_half * cos_ang + lead_half * sin_ang], axis=-1)


def swiglu(rows, w_gate, w_up, w_down):
    gate_val = jnp.dot(rows, w_gate, preferred_element_type=jnp.float32)
    up_val = jnp.dot(rows, w_up, preferred_element_type=jnp.float32)
    act_val = (jax.nn.silu(gate_val) * up_val).astype(jnp.bfloat16)
    return jnp.dot(act_val, w_down, preferred_element_type=jnp.float32)


def attention(normed, cache, kv_lens, w_q, w_uk, w_uv, w_o):
    wq32 = w_q.astype(jnp.float32)
    wuk32 = w_uk.astype(jnp.float32)
    wuv32 = w_uv.astype(jnp.float32)
    wo32 = w_o.astype(jnp.float32)

    def one_token(item):
        vec, kv_rows, length = item
        q_full = jnp.einsum('d,dhc->hc', vec.astype(jnp.float32), wq32).astype(jnp.bfloat16)
        q_rope = rope_rotate(q_full[:, NOPE_DIM:].astype(jnp.float32), length).astype(jnp.bfloat16)
        q_lat = jnp.einsum('hn,hnl->hl', q_full[:, :NOPE_DIM].astype(jnp.float32), wuk32).astype(jnp.bfloat16)
        q_cat = jnp.concatenate([q_lat, q_rope], axis=1)
        scores = jnp.dot(q_cat, kv_rows.T, preferred_element_type=jnp.float32) * SCALE
        valid = jnp.arange(KV_LEN)[None, :] < length
        probs = jax.nn.softmax(jnp.where(valid, scores, -1e30), axis=-1).astype(jnp.bfloat16)
        o_lat = jnp.dot(probs, kv_rows[:, :LATENT], preferred_element_type=jnp.float32).astype(jnp.bfloat16)
        o_val = jnp.einsum('hl,hlv->hv', o_lat.astype(jnp.float32), wuv32).astype(jnp.bfloat16)
        return jnp.einsum('hv,hvd->d', o_val.astype(jnp.float32), wo32)

    return lax.map(one_token, (normed, cache, kv_lens))


def expert_mix(normed, route_ids, route_wts, exp_gate, exp_up, exp_down):
    flat_ids = route_ids.reshape(-1)
    flat_wts = route_wts.reshape(-1)
    num_slots = flat_ids.shape[0]
    key_ids = jnp.where(flat_ids < DEVICES, flat_ids, DEVICES)
    slot_order = jnp.argsort(key_ids, stable=True)
    counts = jax.ops.segment_sum(jnp.ones_like(key_ids), key_ids, num_segments=DEVICES + 1)
    starts = jnp.cumsum(counts) - counts
    local_pos = jnp.arange(ROWS_MAX)

    def one_expert(carry, item):
        start, count, w_gate, w_up, w_down = item
        slot_idx = slot_order[jnp.minimum(start + local_pos, num_slots - 1)]
        tok_idx = slot_idx // TOP_K
        exp_out = swiglu(normed[tok_idx], w_gate, w_up, w_down).astype(jnp.bfloat16)
        slot_wt = jnp.where(local_pos < count, flat_wts[slot_idx], 0.0)
        return carry.at[tok_idx].add(slot_wt[:, None] * exp_out.astype(jnp.float32)), None

    mix_init = jnp.zeros((NUM_TOKENS, HIDDEN), jnp.float32)
    mix, _ = lax.scan(one_expert, mix_init, (starts[:DEVICES], counts[:DEVICES], exp_gate, exp_up, exp_down))
    zero_wt = jnp.sum(jnp.where(route_ids >= DEVICES, route_wts, 0.0), axis=1)
    return mix + zero_wt[:, None] * normed.astype(jnp.float32)


def reference(hidden_in, cache0, cache1, kv_lens, route_ids, route_wts, att0_q, att0_uk, att0_uv, att0_o, att1_q, att1_uk, att1_uv, att1_o, ffn0_gate, ffn0_up, ffn0_down, ffn1_gate, ffn1_up, ffn1_down, exp_gate, exp_up, exp_down):
    att_zero = attention(rms_norm(hidden_in), cache0, kv_lens, att0_q, att0_uk, att0_uv, att0_o)
    h_zero = (hidden_in.astype(jnp.float32) + att_zero).astype(jnp.bfloat16)
    u_zero = rms_norm(h_zero)
    f_zero = (h_zero.astype(jnp.float32) + swiglu(u_zero, ffn0_gate, ffn0_up, ffn0_down)).astype(jnp.bfloat16)
    att_one = attention(rms_norm(f_zero), cache1, kv_lens, att1_q, att1_uk, att1_uv, att1_o)
    h_one = (f_zero.astype(jnp.float32) + att_one).astype(jnp.bfloat16)
    mix = expert_mix(u_zero, route_ids, route_wts, exp_gate, exp_up, exp_down)
    dense_one = swiglu(rms_norm(h_one), ffn1_gate, ffn1_up, ffn1_down)
    return (h_one.astype(jnp.float32) + dense_one + mix).astype(jnp.bfloat16)
```

```python
import functools

import jax
import jax.numpy as jnp
from jax import lax
from jax.experimental import pallas as pl
from jax.experimental.pallas import tpu as pltpu
from jax.sharding import PartitionSpec as P

FLAT_AXES = ('tp', 'ep')
MESH = pl.DeviceIdType.MESH
F32 = jnp.float32
BF16 = jnp.bfloat16
TP = 4
EP = 8
TOK = 32
GROUP = TP * TOK
HID = 2048
SLOTS = 12 * TP
ROWS = EP * SLOTS
FF = 2736
FFP = 2816
FE = 1408
NC = 4
CW = HID // NC
VMEM_LIMIT = 67043328


def rms_norm(vec):
    vec32 = vec.astype(jnp.float32)
    return (vec32 * lax.rsqrt(jnp.mean(vec32 * vec32, axis=-1, keepdims=True) + 1e-6)).astype(jnp.bfloat16)


def rope_rotate(vals, pos):
    half_dim = vals.shape[-1] // 2
    inv_freq = 10000.0 ** (-2.0 * jnp.arange(half_dim, dtype=jnp.float32) / vals.shape[-1])
    rot_angle = pos.astype(jnp.float32)[..., None, None] * inv_freq
    cos_ang = jnp.cos(rot_angle)
    sin_ang = jnp.sin(rot_angle)
    lead_half = vals[..., :half_dim]
    tail_half = vals[..., half_dim:]
    return jnp.concatenate([lead_half * cos_ang - tail_half * sin_ang, tail_half * cos_ang + lead_half * sin_ang], axis=-1)


def attention(normed, cache, kv_lens, w_q, w_uk, w_uv, w_o):
    nope_dim = w_uk.shape[1]
    latent = w_uk.shape[2]
    scale = w_q.shape[2] ** -0.5
    q_full = jnp.einsum('bd,dhc->bhc', normed, w_q, preferred_element_type=jnp.float32).astype(jnp.bfloat16)
    q_rope = rope_rotate(q_full[..., nope_dim:].astype(jnp.float32), kv_lens).astype(jnp.bfloat16)
    q_lat = jnp.einsum('bhn,hnl->bhl', q_full[..., :nope_dim], w_uk, preferred_element_type=jnp.float32).astype(jnp.bfloat16)
    q_cat = jnp.concatenate([q_lat, q_rope], axis=-1)
    scores = jnp.einsum('bhc,bpc->bhp', q_cat, cache, preferred_element_type=jnp.float32) * scale
    valid = jnp.arange(cache.shape[1])[None, None, :] < kv_lens[:, None, None]
    probs = jax.nn.softmax(jnp.where(valid, scores, -1e30), axis=-1).astype(jnp.bfloat16)
    o_lat = jnp.einsum('bhp,bpl->bhl', probs, cache[:, :, :latent], preferred_element_type=jnp.float32).astype(jnp.bfloat16)
    o_val = jnp.einsum('bhl,hlv->bhv', o_lat, w_uv, preferred_element_type=jnp.float32).astype(jnp.bfloat16)
    return jnp.einsum('bhv,hvd->bd', o_val, w_o, preferred_element_type=jnp.float32)


def dot32(a, b):
    return jnp.dot(a, b, preferred_element_type=F32)


def entry_barrier(me_tp, me_ep):
    sem = pltpu.get_barrier_semaphore()
    for k in range(1, TP):
        pl.semaphore_signal(sem, inc=1, device_id={'tp': lax.rem(me_tp + k, TP)}, device_id_type=MESH)
    for k in range(1, EP):
        pl.semaphore_signal(sem, inc=1, device_id={'ep': lax.rem(me_ep + k, EP)}, device_id_type=MESH)
    pl.semaphore_wait(sem, TP + EP - 2)


def load_rows(src, dst, sems, pieces, rows):
    step = rows // pieces
    copies = []
    for i in range(pieces):
        copies.append(pltpu.make_async_copy(src.at[pl.ds(i * step, step)], dst.at[pl.ds(i * step, step)], sems.at[i]))
    for c in copies:
        c.start()
    return copies


def wait_all(copies):
    for c in copies:
        c.wait()


def send_tp(src, dst, ssem, rsem, k, me_tp):
    return pltpu.make_async_remote_copy(src_ref=src, dst_ref=dst, send_sem=ssem, recv_sem=rsem,
                                        device_id={'tp': lax.rem(me_tp + k, TP)}, device_id_type=MESH)


def send_ep(src, dst, ssem, rsem, k, me_ep):
    return pltpu.make_async_remote_copy(src_ref=src, dst_ref=dst, send_sem=ssem, recv_sem=rsem,
                                        device_id={'ep': lax.rem(me_ep + k, EP)}, device_id_type=MESH)


def route_tables(ids_t, me_tp):
    members = []
    for e in range(EP):
        hit = (ids_t == me_tp * EP + e).astype(F32)
        members.append(jnp.sum(hit, axis=0, keepdims=True))
    member = jnp.concatenate(members, axis=0)
    before = (lax.broadcasted_iota(jnp.int32, (GROUP, GROUP), 0) < lax.broadcasted_iota(jnp.int32, (GROUP, GROUP), 1))
    rank = dot32(member.astype(BF16), before.astype(F32).astype(BF16))
    slot = lax.broadcasted_iota(jnp.int32, (SLOTS, GROUP), 0).astype(F32)
    picks = []
    for e in range(EP):
        hit = jnp.logical_and(rank[e:e + 1, :] == slot, member[e:e + 1, :] > 0.5)
        picks.append(hit.astype(F32))
    return picks


def gated(rows, gbuf, ubuf, act, total, tile):
    n0 = 0
    while n0 < total:
        width = min(tile, total - n0)
        g = dot32(rows, gbuf[:, n0:n0 + width])
        u = dot32(rows, ubuf[:, n0:n0 + width])
        act[:, n0:n0 + width] = (jax.nn.silu(g) * u).astype(BF16)
        n0 += width


def ffn0_kernel(h_ref, ids_ref, wts_ref, g_hbm, u_hbm, d_hbm,
                f_ref, unorm_ref, rows_ref, idsg_ref, wtsg_ref,
                uall, idsall, wtsall, gbuf, ubuf, dbuf, act, part, rs, sendb, recvb,
                wsem, ag_s, ag_r, rt_s, rt_r, rs_s, rs_r, dp_s, dp_r, lsem):
    me_tp = lax.axis_index('tp')
    me_ep = lax.axis_index('ep')
    wg = load_rows(g_hbm, gbuf, wsem.at[0], 4, HID)
    wu = load_rows(u_hbm, ubuf, wsem.at[1], 4, HID)
    wd = load_rows(d_hbm, dbuf, wsem.at[2], 3, FF)
    unorm = rms_norm(h_ref[...])
    unorm_ref[...] = unorm
    uall[me_tp] = unorm
    idsall[me_tp] = ids_ref[...]
    wtsall[me_tp] = wts_ref[...]
    entry_barrier(me_tp, me_ep)
    ag = []
    for k in (2, 1, 3):
        ag.append(send_tp(uall.at[me_tp], uall.at[me_tp], ag_s.at[k - 1], ag_r.at[k - 1], k, me_tp))
    rt = []
    for k in (1, 2, 3):
        rt.append(send_tp(ids_ref, idsall.at[me_tp], rt_s.at[0, k - 1], rt_r.at[0, k - 1], k, me_tp))
        rt.append(send_tp(wts_ref, wtsall.at[me_tp], rt_s.at[1, k - 1], rt_r.at[1, k - 1], k, me_tp))
    for c in rt + ag:
        c.start()
    dbuf[FF:, :] = jnp.zeros((FFP - FF, HID), BF16)
    act[:, FF:] = jnp.zeros((GROUP, FFP - FF), BF16)
    wait_all(rt)
    picks = route_tables(idsall[...].reshape(GROUP, 128).T, me_tp)
    idsg_ref[...] = idsall[...]
    wtsg_ref[...] = wtsall[...]
    wait_all(ag)
    rows = uall[...].reshape(GROUP, HID)
    for e in range(EP):
        sendb[e] = dot32(picks[e].astype(BF16), rows).astype(BF16)
    dp = []
    for k in (7, 6, 5, 4, 3, 2, 1):
        dp.append(send_ep(sendb.at[lax.rem(me_ep + k, EP)], recvb.at[me_ep], dp_s.at[k - 1], dp_r.at[k - 1], k, me_ep))
    for c in dp:
        c.start()
    own = pltpu.make_async_copy(sendb.at[me_ep], recvb.at[me_ep], lsem.at[0])
    own.start()
    wait_all(wg)
    wait_all(wu)
    gated(rows, gbuf, ubuf, act, FF, 512)
    wait_all(wd)
    rss = []
    for c in range(NC):
        part[c] = dot32(act[...], dbuf[:, c * CW:(c + 1) * CW]).reshape(TP, TOK, CW)
        for k in (2, 1, 3):
            copy = send_tp(part.at[c, lax.rem(me_tp + k, TP)], rs.at[c, k - 1], rs_s.at[c, k - 1], rs_r.at[c, k - 1], k, me_tp)
            copy.start()
            rss.append(copy)
    own.wait()
    wait_all(dp)
    out = pltpu.make_async_copy(recvb, rows_ref, lsem.at[1])
    out.start()
    wait_all(rss)
    for c in range(NC):
        total = part[c, me_tp] + rs[c, 0] + rs[c, 1] + rs[c, 2]
        cols = slice(c * CW, (c + 1) * CW)
        f_ref[:, cols] = (h_ref[:, cols].astype(F32) + total).astype(BF16)
    out.wait()


def ffn1_kernel(h_ref, u0_ref, ids_ref, wts_ref, idsg_ref, wtsg_ref, rows_ref, eg_hbm, eu_hbm, ed_hbm, g_hbm, u_hbm, d_hbm,
                y_ref,
                uall, gbuf, ubuf, dbuf, act, part, rs, egbuf, eubuf, edbuf, acte, eo, comb,
                wsem, ag_s, ag_r, rs_s, rs_r, cb_s, cb_r, lsem):
    me_tp = lax.axis_index('tp')
    me_ep = lax.axis_index('ep')
    weg = load_rows(eg_hbm.at[0], egbuf, wsem.at[3], 2, HID)
    weu = load_rows(eu_hbm.at[0], eubuf, wsem.at[4], 2, HID)
    wed = load_rows(ed_hbm.at[0], edbuf, wsem.at[5], 2, FE)
    wg = load_rows(g_hbm, gbuf, wsem.at[0], 4, HID)
    wu = load_rows(u_hbm, ubuf, wsem.at[1], 4, HID)
    wd = load_rows(d_hbm, dbuf, wsem.at[2], 3, FF)
    uall[me_tp] = rms_norm(h_ref[...])
    entry_barrier(me_tp, me_ep)
    ag = []
    for k in (2, 1, 3):
        ag.append(send_tp(uall.at[me_tp], uall.at[me_tp], ag_s.at[k - 1], ag_r.at[k - 1], k, me_tp))
    for c in ag:
        c.start()
    dbuf[FF:, :] = jnp.zeros((FFP - FF, HID), BF16)
    act[:, FF:] = jnp.zeros((GROUP, FFP - FF), BF16)
    wait_all(weg)
    wait_all(weu)
    gated(rows_ref[...].reshape(ROWS, HID), egbuf, eubuf, acte, FE, 512)
    wait_all(wed)
    cbs = []
    owns = []
    for c in range(NC):
        eo[c] = dot32(acte[...], edbuf[:, c * CW:(c + 1) * CW]).astype(BF16).reshape(EP, SLOTS, CW)
        group = []
        for k in (7, 6, 5, 4, 3, 2, 1):
            copy = send_ep(eo.at[c, lax.rem(me_ep + k, EP)], comb.at[c, me_ep], cb_s.at[c, k - 1], cb_r.at[c, k - 1], k, me_ep)
            copy.start()
            group.append(copy)
        cbs.append(group)
        own = pltpu.make_async_copy(eo.at[c, me_ep], comb.at[c, me_ep], lsem.at[c])
        own.start()
        owns.append(own)
    ids_t = idsg_ref[...].reshape(GROUP, 128).T
    wts_t = wtsg_ref[...].reshape(GROUP, 128).T
    picks = route_tables(ids_t, me_tp)
    weighted = []
    for e in range(EP):
        wsel = jnp.sum(jnp.where(ids_t == me_tp * EP + e, wts_t, 0.0), axis=0, keepdims=True)
        weighted.append(picks[e] * wsel)
    mix = jnp.concatenate(weighted, axis=0).T
    mix_hi = mix.astype(BF16)
    rest = mix - mix_hi.astype(F32)
    mix_mid = rest.astype(BF16)
    mix_lo = (rest - mix_mid.astype(F32)).astype(BF16)
    wait_all(ag)
    wait_all(wg)
    wait_all(wu)
    gated(uall[...].reshape(GROUP, HID), gbuf, ubuf, act, FF, 512)
    wait_all(wd)
    rss = []
    for c in range(NC):
        total = dot32(act[...], dbuf[:, c * CW:(c + 1) * CW])
        wait_all(cbs[c])
        owns[c].wait()
        back = comb[c].reshape(ROWS, CW)
        total = total + (dot32(mix_lo, back) + dot32(mix_mid, back) + dot32(mix_hi, back))
        part[c] = total.reshape(TP, TOK, CW)
        for k in (2, 1, 3):
            copy = send_tp(part.at[c, lax.rem(me_tp + k, TP)], rs.at[c, k - 1], rs_s.at[c, k - 1], rs_r.at[c, k - 1], k, me_tp)
            copy.start()
            rss.append(copy)
    zero_wt = jnp.sum(jnp.where(ids_ref[...] >= TP * EP, wts_ref[...], 0.0), axis=1, keepdims=True)
    wait_all(rss)
    for c in range(NC):
        cols = slice(c * CW, (c + 1) * CW)
        total = part[c, me_tp] + rs[c, 0] + rs[c, 1] + rs[c, 2] + zero_wt * u0_ref[:, cols].astype(F32)
        y_ref[:, cols] = (h_ref[:, cols].astype(F32) + total).astype(BF16)


VM = pl.BlockSpec(memory_space=pltpu.VMEM)
ANY = pl.BlockSpec(memory_space=pl.ANY)
DMA = pltpu.SemaphoreType.DMA


def call_ffn0(h, ids, wts, g, u, d):
    sds = jax.ShapeDtypeStruct
    return pl.pallas_call(
        ffn0_kernel,
        name='ffn0',
        out_shape=(sds((TOK, HID), BF16), sds((TOK, HID), BF16), sds((EP, SLOTS, HID), BF16),
                   sds((TP, TOK, 128), jnp.int32), sds((TP, TOK, 128), F32)),
        in_specs=[VM, VM, VM, ANY, ANY, ANY],
        out_specs=(VM, VM, ANY, VM, VM),
        scratch_shapes=[
            pltpu.VMEM((TP, TOK, HID), BF16), pltpu.VMEM((TP, TOK, 128), jnp.int32), pltpu.VMEM((TP, TOK, 128), F32),
            pltpu.VMEM((HID, FF), BF16), pltpu.VMEM((HID, FF), BF16), pltpu.VMEM((FFP, HID), BF16),
            pltpu.VMEM((GROUP, FFP), BF16), pltpu.VMEM((NC, TP, TOK, CW), F32), pltpu.VMEM((NC, TP - 1, TOK, CW), F32),
            pltpu.VMEM((EP, SLOTS, HID), BF16), pltpu.VMEM((EP, SLOTS, HID), BF16),
            DMA((3, 4)), DMA((3,)), DMA((3,)), DMA((2, 3)), DMA((2, 3)), DMA((NC, 3)), DMA((NC, 3)), DMA((7,)), DMA((7,)), DMA((2,)),
        ],
        compiler_params=pltpu.CompilerParams(collective_id=0, has_side_effects=True, vmem_limit_bytes=VMEM_LIMIT),
    )(h, ids, wts, g, u, d)


def call_ffn1(h, u0, ids, wts, idsg, wtsg, rows, eg, eu, ed, g, u, d):
    return pl.pallas_call(
        ffn1_kernel,
        name='ffn1',
        out_shape=jax.ShapeDtypeStruct((TOK, HID), BF16),
        in_specs=[VM] * 7 + [ANY] * 6,
        out_specs=VM,
        scratch_shapes=[
            pltpu.VMEM((TP, TOK, HID), BF16),
            pltpu.VMEM((HID, FF), BF16), pltpu.VMEM((HID, FF), BF16), pltpu.VMEM((FFP, HID), BF16),
            pltpu.VMEM((GROUP, FFP), BF16), pltpu.VMEM((NC, TP, TOK, CW), F32), pltpu.VMEM((NC, TP - 1, TOK, CW), F32),
            pltpu.VMEM((HID, FE), BF16), pltpu.VMEM((HID, FE), BF16), pltpu.VMEM((FE, HID), BF16),
            pltpu.VMEM((ROWS, FE), BF16), pltpu.VMEM((NC, EP, SLOTS, CW), BF16), pltpu.VMEM((NC, EP, SLOTS, CW), BF16),
            DMA((6, 4)), DMA((3,)), DMA((3,)), DMA((NC, 3)), DMA((NC, 3)), DMA((NC, 7)), DMA((NC, 7)), DMA((NC,)),
        ],
        compiler_params=pltpu.CompilerParams(collective_id=1, has_side_effects=True, vmem_limit_bytes=VMEM_LIMIT),
    )(h, u0, ids, wts, idsg, wtsg, rows, eg, eu, ed, g, u, d)


def solution(mesh):
    rows_spec = P(FLAT_AXES, None)
    cube_spec = P(FLAT_AXES, None, None)
    whole_spec = P(None, None, None)
    col_split = P(None, 'tp')
    row_split = P('tp', None)
    in_specs = (rows_spec, cube_spec, cube_spec, P(FLAT_AXES), rows_spec, rows_spec,
                whole_spec, whole_spec, whole_spec, whole_spec, whole_spec, whole_spec, whole_spec, whole_spec,
                col_split, col_split, row_split, col_split, col_split, row_split,
                cube_spec, cube_spec, cube_spec)

    def body(hidden_in, cache0, cache1, kv_lens, route_ids, route_wts, att0_q, att0_uk, att0_uv, att0_o, att1_q, att1_uk, att1_uv, att1_o, ffn0_gate, ffn0_up, ffn0_down, ffn1_gate, ffn1_up, ffn1_down, exp_gate, exp_up, exp_down):
        ids = jnp.pad(route_ids, ((0, 0), (0, 122)), constant_values=-1)
        wts = jnp.pad(route_wts, ((0, 0), (0, 122)))
        att_zero = attention(rms_norm(hidden_in), cache0, kv_lens, att0_q, att0_uk, att0_uv, att0_o)
        h_zero = (hidden_in.astype(jnp.float32) + att_zero).astype(jnp.bfloat16)
        f_zero, u_zero, rows, idsg, wtsg = call_ffn0(h_zero, ids, wts, ffn0_gate, ffn0_up, ffn0_down)
        att_one = attention(rms_norm(f_zero), cache1, kv_lens, att1_q, att1_uk, att1_uv, att1_o)
        h_one = (f_zero.astype(jnp.float32) + att_one).astype(jnp.bfloat16)
        return call_ffn1(h_one, u_zero, ids, wts, idsg, wtsg, rows, exp_gate, exp_up, exp_down, ffn1_gate, ffn1_up, ffn1_down)

    return jax.shard_map(body, mesh=mesh, in_specs=in_specs, out_specs=rows_spec, check_vma=False)
```

```python
import jax
import jax.numpy as jnp
from jax import lax
from jax.experimental import pallas as pl
from jax.experimental.pallas import tpu as pltpu
from jax.sharding import PartitionSpec as P

FLAT_AXES = ('tp', 'ep')
MESH = pl.DeviceIdType.MESH
F32 = jnp.float32
BF16 = jnp.bfloat16
TP = 4
EP = 8
TOK = 32
TOP_K = 6
GROUP = TP * TOK
HID = 2048
SLOTS = 12 * TP
ROWS = EP * SLOTS
FF = 2736
FFP = 2816
FE = 1408
EB = 256
NEB = -(-FE // EB)
NC = 4
CW = HID // NC
HEADS = 16
NOPE = 128
ROPE = 64
QK = NOPE + ROPE
VDIM = 128
LAT = 512
LT = LAT // 128
KV = 256
CD = LAT + ROPE
CGRP = 8
NGRP = TOK // CGRP
QROWS = HEADS * QK
R_Q = 0
R_U = 0
R_O = QROWS
R_D = QROWS
R_G = R_D + FFP
WROWS = R_G + FF
VMEM_LIMIT = 67043328


def rms_norm(vec):
    vec32 = vec.astype(F32)
    return (vec32 * lax.rsqrt(jnp.mean(vec32 * vec32, axis=-1, keepdims=True) + 1e-6)).astype(BF16)


def dot32(a, b):
    return jnp.dot(a, b, preferred_element_type=F32)


def dot_nt(a, b):
    return lax.dot_general(a, b, (((1,), (1,)), ((), ())), preferred_element_type=F32)


def start_all(copies):
    for c in copies:
        c.start()


def wait_all(copies):
    for c in copies:
        c.wait()


def row_copies(src, dst, sems, pieces, rows):
    step = rows // pieces
    return [pltpu.make_async_copy(src.at[pl.ds(i * step, step)], dst.at[pl.ds(i * step, step)], sems.at[i]) for i in range(pieces)]


def send_to(axis, pos, src, dst, ssem, rsem):
    return pltpu.make_async_remote_copy(src_ref=src, dst_ref=dst, send_sem=ssem, recv_sem=rsem,
                                        device_id={axis: pos}, device_id_type=MESH)


def entry_barrier(me_tp, me_ep):
    sem = pltpu.get_barrier_semaphore()
    for k in range(1, TP):
        pl.semaphore_signal(sem, inc=1, device_id={'tp': lax.rem(me_tp + k, TP)}, device_id_type=MESH)
    for k in range(1, EP):
        pl.semaphore_signal(sem, inc=1, device_id={'ep': lax.rem(me_ep + k, EP)}, device_id_type=MESH)
    pl.semaphore_wait(sem, TP + EP - 2)


def route_picks(ids_t, me_tp):
    members = [jnp.sum((ids_t == me_tp * EP + e).astype(F32), axis=0, keepdims=True) for e in range(EP)]
    member = jnp.concatenate(members, axis=0)
    before = (lax.broadcasted_iota(jnp.int32, (GROUP, GROUP), 0) < lax.broadcasted_iota(jnp.int32, (GROUP, GROUP), 1))
    rank = dot32(member.astype(BF16), before.astype(F32).astype(BF16))
    slot = lax.broadcasted_iota(jnp.int32, (SLOTS, GROUP), 0).astype(F32)
    return [jnp.logical_and(rank[e:e + 1, :] == slot, member[e:e + 1, :] > 0.5).astype(F32) for e in range(EP)]


def gated_nt(rows, wb, act):
    n0 = 0
    while n0 < FF:
        width = min(512, FF - n0)
        g = dot_nt(rows[...].reshape(GROUP, HID), wb[R_G + n0:R_G + n0 + width, :])
        u = dot_nt(rows[...].reshape(GROUP, HID), wb[R_U + n0:R_U + n0 + width, :])
        act[:, n0:n0 + width] = (jax.nn.silu(g) * u).astype(BF16)
        n0 += width


def rotary(lens_ref):
    lane = lax.broadcasted_iota(jnp.int32, (ROPE // 2, 128), 1)
    half = lax.broadcasted_iota(jnp.int32, (ROPE // 2, 128), 0).astype(F32)
    pos = jnp.zeros((ROPE // 2, 128), F32)
    for t in range(TOK):
        pos = jnp.where(lane == t, lens_ref[t].astype(F32), pos)
    angle = pos * jnp.exp(half * (-2.0 / ROPE * 9.210340371976184))
    return jnp.cos(angle), jnp.sin(angle)


def attention(h, lens_ref, wq, uk, caches, uv, wo, wb, ukb, uvb, kvb, qc, after_q, after_group):
    normed = rms_norm(h)
    cos_t, sin_t = rotary(lens_ref)
    uk.wait()
    piece = QROWS // 4
    for i in range(4):
        wq[i].wait()
        q = dot_nt(normed, wb[R_Q + i * piece:R_Q + (i + 1) * piece, :]).astype(BF16).astype(F32)
        q_t = jnp.concatenate([q, jnp.zeros((128 - TOK, piece), F32)], axis=0).T
        for j in range(4):
            head = i * 4 + j
            base = j * QK
            q_n = q_t[base:base + NOPE, :].T[:TOK, :].astype(BF16)
            lead = q_t[base + NOPE:base + NOPE + ROPE // 2, :]
            tail = q_t[base + NOPE + ROPE // 2:base + QK, :]
            rot = jnp.concatenate([lead * cos_t - tail * sin_t, tail * cos_t + lead * sin_t,
                                   jnp.zeros((128 - ROPE, 128), F32)], axis=0).T[:TOK, :]
            q_lat = dot32(q_n, ukb[head * NOPE:(head + 1) * NOPE, :])
            for l in range(LT):
                qc[l, pl.ds(head, TOK, stride=HEADS), :] = q_lat[:, l * 128:(l + 1) * 128]
            qc[LT, pl.ds(head, TOK, stride=HEADS), :] = rot
    after_q()
    position = lax.broadcasted_iota(jnp.int32, (HEADS, KV), 1)
    for g in range(NGRP):
        caches[g].wait()
        toks = range(g * CGRP, (g + 1) * CGRP)
        scores = []
        for t in toks:
            q_cat = jnp.concatenate([qc[l, t * HEADS:(t + 1) * HEADS, :] for l in range(LT + 1)], axis=1)[:, :CD].astype(BF16)
            scores.append(dot32(q_cat, kvb[t * CD:(t + 1) * CD, :]) * (QK ** -0.5))
        probs = []
        for t, s in zip(toks, scores):
            s = jnp.where(position < lens_ref[t], s, -1e30)
            ex = jnp.exp(s - jnp.max(s, axis=-1, keepdims=True))
            probs.append((ex / jnp.sum(ex, axis=-1, keepdims=True)).astype(BF16))
        for t, p in zip(toks, probs):
            o_tok = dot_nt(p, kvb[t * CD:t * CD + LAT, :])
            for l in range(LT):
                qc[l, t * HEADS:(t + 1) * HEADS, :] = o_tok[:, l * 128:(l + 1) * 128]
        after_group(g)
    uv.wait()
    vals = []
    for head in range(HEADS):
        o_lat = jnp.concatenate([qc[l, pl.ds(head, TOK, stride=HEADS), :] for l in range(LT)], axis=1).astype(BF16)
        vals.append(dot32(o_lat, uvb[head * LAT:(head + 1) * LAT, :]).astype(BF16))
    o_val = jnp.concatenate(vals, axis=1)
    wo.wait()
    return dot32(o_val, wb[R_O:R_O + HID, :])


class LineReduce:
    def __init__(self, part, rs, ssem, rsem, me):
        self.part, self.rs, self.ssem, self.rsem, self.me = part, rs, ssem, rsem, me

    def copy(self, way, c, dest):
        slot = dest - 1 if way == 0 else dest
        nxt = lax.rem(self.me + (1 if way == 0 else TP - 1), TP)
        return send_to('tp', nxt, self.part.at[c, dest], self.rs.at[way, c, slot], self.ssem.at[way, c, slot], self.rsem.at[way, c, slot])

    def absorb(self, way, c, dest):
        slot = dest - 1 if way == 0 else dest
        self.copy(way, c, dest).wait_recv()
        self.part[c, dest] = self.part[c, dest] + self.rs[way, c, slot]

    def ends(self, c):
        @pl.when(self.me == 0)
        def _():
            self.copy(0, c, TP - 1).start()

        @pl.when(self.me == TP - 1)
        def _():
            self.copy(1, c, 0).start()

    def step(self, r, c):
        me = self.me

        @pl.when(me + r <= TP - 1)
        def _():
            @pl.when(me > 0)
            def _():
                self.absorb(0, c, me + r)
            self.copy(0, c, me + r).start()

        @pl.when(me - r >= 0)
        def _():
            @pl.when(me < TP - 1)
            def _():
                self.absorb(1, c, me - r)
            self.copy(1, c, me - r).start()

    def finish(self, c):
        me = self.me

        @pl.when(me > 0)
        def _():
            self.absorb(0, c, me)

        @pl.when(me < TP - 1)
        def _():
            self.absorb(1, c, me)
        return self.part[c, me]

    def drain(self):
        me = self.me
        for r in range(1, TP):
            @pl.when(me + r <= TP - 1)
            def _():
                for c in range(NC):
                    self.copy(0, c, me + r).wait_send()

            @pl.when(me - r >= 0)
            def _():
                for c in range(NC):
                    self.copy(1, c, me - r).wait_send()


def gather_rows(uall, ssem, rsem, me_tp):
    copies = [send_to('tp', lax.rem(me_tp + k, TP), uall.at[me_tp], uall.at[me_tp], ssem.at[k - 1], rsem.at[k - 1]) for k in (2, 1, 3)]
    start_all(copies)
    return copies


def layer_kernel(lens_ref, x_ref, ids_ref, wts_ref,
                 q0, uk0, uv0, o0, c0, q1, uk1, uv1, o1, c1, g0, u0, d0, g1, u1, d1, eg, eu, ed,
                 y_ref,
                 wb, ukb, uvb, kvb, qc, uall, act, part, rs, eo, recvb, comb, acte, routes, routeg, hbuf, ubuf,
                 qsem, csem, asem, wsem, esem, ag_s, ag_r, rt_s, rt_r, rs_s, rs_r, dp_s, dp_r, cb_s, cb_r, lsem):
    me_tp = lax.axis_index('tp')
    me_ep = lax.axis_index('ep')

    def att_copies(n, q, uk, uv, o, c):
        wq = row_copies(q, wb.at[pl.ds(R_Q, QROWS)], qsem.at[n], 4, QROWS)
        ukc = pltpu.make_async_copy(uk, ukb, asem.at[n, 0])
        uvc = pltpu.make_async_copy(uv, uvb, asem.at[n, 1])
        wo = pltpu.make_async_copy(o, wb.at[pl.ds(R_O, HID)], asem.at[n, 2])
        step = CGRP * CD
        kv = [pltpu.make_async_copy(c.at[pl.ds(g * step, step)], kvb.at[pl.ds(g * step, step)], csem.at[n, g]) for g in range(NGRP)]
        return wq, ukc, kv, uvc, wo

    def ffn_copies(n, g, u, d):
        return (row_copies(g, wb.at[pl.ds(R_G, FF)], wsem.at[n, 0], 3, FF), row_copies(u, wb.at[pl.ds(R_U, FF)], wsem.at[n, 1], 3, FF),
                row_copies(d, wb.at[pl.ds(R_D, FF)], wsem.at[n, 2], 3, FF))

    def expert_copies(src, which):
        copies = []
        for b in range(NEB):
            width = min(EB, FE - b * EB)
            row = (which * NEB + b) * HID
            copies.append(pltpu.make_async_copy(src.at[0, :, pl.ds(b * EB, width)], kvb.at[pl.ds(row, HID), pl.ds(0, width)], esem.at[which, b]))
        return copies

    wq, ukc, kv, uvc, wo = att_copies(0, q0, uk0, uv0, o0, c0)
    wg, wu, wd = ffn_copies(0, g0, u0, d0)
    weg = expert_copies(eg, 0)
    weu = expert_copies(eu, 1)
    wed = row_copies(ed.at[0], wb.at[pl.ds(R_G, FE)], esem.at[2], 2, FE)
    ukc.start()
    start_all(wq)
    start_all(kv)
    uvc.start()
    wo.start()
    start_all(wg)

    routes[...] = jnp.full((2, 8, 128), -1.0, F32)
    routes[0, :TOP_K, :TOK] = ids_ref[...].astype(F32)
    routes[1, :TOP_K, :TOK] = wts_ref[...]
    routeg[me_tp] = routes[...]
    entry_barrier(me_tp, me_ep)
    rt = [send_to('tp', lax.rem(me_tp + k, TP), routes, routeg.at[me_tp], rt_s.at[k - 1], rt_r.at[k - 1]) for k in (1, 2, 3)]
    start_all(rt)

    def after_q0():
        start_all(wu)

    def after_group0(g):
        if g == NGRP - 1:
            start_all(weg)
            start_all(weu)

    att = attention(x_ref[...], lens_ref, wq, ukc, kv, uvc, wo, wb, ukb, uvb, kvb, qc, after_q0, after_group0)
    h = (x_ref[...].astype(F32) + att).astype(BF16)
    hbuf[...] = h
    start_all(wd)
    unorm = rms_norm(h)
    ubuf[...] = unorm
    uall[me_tp] = unorm
    ag = gather_rows(uall, ag_s.at[0], ag_r.at[0], me_tp)
    wb[R_D + FF:R_D + FFP, :] = jnp.zeros((FFP - FF, HID), BF16)
    act[:, FF:] = jnp.zeros((GROUP, FFP - FF), BF16)
    wait_all(rt)
    ids_t = jnp.concatenate([routeg[z, 0, :TOP_K, :TOK] for z in range(TP)], axis=1).astype(jnp.int32)
    picks = route_picks(ids_t, me_tp)
    wait_all(ag)
    for e in range(EP):
        eo[e] = dot32(picks[e].astype(BF16), uall[...].reshape(GROUP, HID)).astype(BF16)
    dp = []
    for k in (7, 6, 5, 4, 3, 2, 1):
        peer = lax.rem(me_ep + k, EP)
        dp.append(send_to('ep', peer, eo.at[peer], recvb.at[me_ep], dp_s.at[k - 1], dp_r.at[k - 1]))
    start_all(dp)
    own_rows = pltpu.make_async_copy(eo.at[me_ep], recvb.at[me_ep], lsem.at[NC])
    own_rows.start()
    wait_all(wg)
    wait_all(wu)
    gated_nt(uall, wb, act)
    wait_all(wd)
    start_all(wed)
    wq, ukc, kv, uvc, wo = att_copies(1, q1, uk1, uv1, o1, c1)
    wg, wu, wd = ffn_copies(1, g1, u1, d1)
    ukc.start()
    start_all(wq)
    uvc.start()
    line = LineReduce(part, rs, rs_s.at[0], rs_r.at[0], me_tp)
    for c in range(NC):
        part[c] = dot32(act[...], wb[R_D:R_D + FFP, c * CW:(c + 1) * CW]).reshape(TP, TOK, CW)
        line.ends(c)
    wo.start()
    for c in range(NC):
        line.step(2, c)
    own_rows.wait()
    wait_all(dp)
    wait_all(weg)
    wait_all(weu)
    for b in range(NEB):
        width = min(EB, FE - b * EB)
        g = dot32(recvb[...].reshape(ROWS, HID), kvb[b * HID:(b + 1) * HID, :width])
        u = dot32(recvb[...].reshape(ROWS, HID), kvb[(NEB + b) * HID:(NEB + b + 1) * HID, :width])
        acte[:, b * EB:b * EB + width] = (jax.nn.silu(g) * u).astype(BF16)
        if 1 <= b <= NC:
            line.step(1, b - 1)
    start_all(kv)
    wait_all(wed)
    cbs = []
    for c in range(NC):
        cols = pl.ds(c * CW, CW)
        eo[:, :, c * CW:(c + 1) * CW] = dot32(acte[...], wb[R_G:R_G + FE, c * CW:(c + 1) * CW]).astype(BF16).reshape(EP, SLOTS, CW)
        for k in (7, 6, 5, 4, 3, 2, 1):
            peer = lax.rem(me_ep + k, EP)
            cbs.append(send_to('ep', peer, eo.at[peer, :, cols], comb.at[c, me_ep], cb_s.at[c, k - 1], cb_r.at[c, k - 1]))
            cbs[-1].start()
        own = pltpu.make_async_copy(eo.at[me_ep, :, cols], comb.at[c, me_ep], lsem.at[c])
        own.start()
        cbs.append(own)
    start_all(wg)
    for c in range(NC):
        cols = slice(c * CW, (c + 1) * CW)
        hbuf[:, cols] = (hbuf[:, cols].astype(F32) + line.finish(c)).astype(BF16)
    line.drain()

    def after_q1():
        start_all(wu)

    def after_group1(g):
        pass

    att = attention(hbuf[...], lens_ref, wq, ukc, kv, uvc, wo, wb, ukb, uvb, kvb, qc, after_q1, after_group1)
    h = (hbuf[...].astype(F32) + att).astype(BF16)
    hbuf[...] = h
    start_all(wd)
    uall[me_tp] = rms_norm(h)
    ag = gather_rows(uall, ag_s.at[1], ag_r.at[1], me_tp)
    wb[R_D + FF:R_D + FFP, :] = jnp.zeros((FFP - FF, HID), BF16)
    ids_t = jnp.concatenate([routeg[z, 0, :TOP_K, :TOK] for z in range(TP)], axis=1).astype(jnp.int32)
    wts_t = jnp.concatenate([routeg[z, 1, :TOP_K, :TOK] for z in range(TP)], axis=1)
    picks = route_picks(ids_t, me_tp)
    weighted = []
    for e in range(EP):
        wsel = jnp.sum(jnp.where(ids_t == me_tp * EP + e, wts_t, 0.0), axis=0, keepdims=True)
        weighted.append(picks[e] * wsel)
    mix = jnp.concatenate(weighted, axis=0).T
    mix_hi = mix.astype(BF16)
    rest = mix - mix_hi.astype(F32)
    mix_mid = rest.astype(BF16)
    mix_lo = (rest - mix_mid.astype(F32)).astype(BF16)
    wait_all(cbs)
    for c in range(NC):
        back = comb[c].reshape(ROWS, CW)
        part[c] = (dot32(mix_lo, back) + dot32(mix_mid, back) + dot32(mix_hi, back)).reshape(TP, TOK, CW)
    wait_all(ag)
    wait_all(wg)
    wait_all(wu)
    gated_nt(uall, wb, act)
    wait_all(wd)
    line = LineReduce(part, rs, rs_s.at[1], rs_r.at[1], me_tp)
    for c in range(NC):
        part[c] = part[c] + dot32(act[...], wb[R_D:R_D + FFP, c * CW:(c + 1) * CW]).reshape(TP, TOK, CW)
        line.ends(c)
    for c in range(NC):
        line.step(2, c)
    for c in range(NC):
        line.step(1, c)
    own_ids = routes[0].T[:TOK, :]
    own_wts = routes[1].T[:TOK, :]
    zero_wt = jnp.sum(jnp.where(own_ids >= TP * EP, own_wts, 0.0), axis=1, keepdims=True)
    for c in range(NC):
        cols = slice(c * CW, (c + 1) * CW)
        total = line.finish(c) + zero_wt * ubuf[:, cols].astype(F32)
        y_ref[:, cols] = (hbuf[:, cols].astype(F32) + total).astype(BF16)
    line.drain()


VM = pl.BlockSpec(memory_space=pltpu.VMEM)
ANY = pl.BlockSpec(memory_space=pl.ANY)
DMA = pltpu.SemaphoreType.DMA


def call_layer(*args):
    return pl.pallas_call(
        layer_kernel,
        name='layer',
        out_shape=jax.ShapeDtypeStruct((TOK, HID), BF16),
        in_specs=[pl.BlockSpec(memory_space=pltpu.SMEM)] + [VM] * 3 + [ANY] * 19,
        out_specs=VM,
        scratch_shapes=[
            pltpu.VMEM((WROWS, HID), BF16), pltpu.VMEM((HEADS * NOPE, LAT), BF16), pltpu.VMEM((HEADS * LAT, VDIM), BF16),
            pltpu.VMEM((2 * NEB * HID, KV), BF16), pltpu.VMEM((LT + 1, TOK * HEADS, 128), F32),
            pltpu.VMEM((TP, TOK, HID), BF16), pltpu.VMEM((GROUP, FFP), BF16),
            pltpu.VMEM((NC, TP, TOK, CW), F32), pltpu.VMEM((2, NC, TP - 1, TOK, CW), F32),
            pltpu.VMEM((EP, SLOTS, HID), BF16), pltpu.VMEM((EP, SLOTS, HID), BF16), pltpu.VMEM((NC, EP, SLOTS, CW), BF16),
            pltpu.VMEM((ROWS, FE), BF16), pltpu.VMEM((2, 8, 128), F32), pltpu.VMEM((TP, 2, 8, 128), F32),
            pltpu.VMEM((TOK, HID), BF16), pltpu.VMEM((TOK, HID), BF16),
            DMA((2, 4)), DMA((2, NGRP)), DMA((2, 3)), DMA((2, 3, 3)), DMA((3, NEB)),
            DMA((2, 3)), DMA((2, 3)), DMA((3,)), DMA((3,)),
            DMA((2, 2, NC, 3)), DMA((2, 2, NC, 3)), DMA((7,)), DMA((7,)), DMA((NC, 7)), DMA((NC, 7)), DMA((NC + 1,)),
        ],
        compiler_params=pltpu.CompilerParams(collective_id=0, has_side_effects=True, vmem_limit_bytes=VMEM_LIMIT),
    )(*args)


def attention_operands(q, uk, uv, o, cache):
    return (q.transpose(1, 2, 0).reshape(QROWS, HID), uk.reshape(HEADS * NOPE, LAT), uv.reshape(HEADS * LAT, VDIM),
            o.reshape(HEADS * VDIM, HID), cache.transpose(0, 2, 1).reshape(TOK * CD, KV))


def solution(mesh):
    rows_spec = P(FLAT_AXES, None)
    cube_spec = P(FLAT_AXES, None, None)
    whole_spec = P(None, None, None)
    col_split = P(None, 'tp')
    row_split = P('tp', None)
    in_specs = (rows_spec, cube_spec, cube_spec, P(FLAT_AXES), rows_spec, rows_spec,
                whole_spec, whole_spec, whole_spec, whole_spec, whole_spec, whole_spec, whole_spec, whole_spec,
                col_split, col_split, row_split, col_split, col_split, row_split,
                cube_spec, cube_spec, cube_spec)

    def body(hidden_in, cache0, cache1, kv_lens, route_ids, route_wts, att0_q, att0_uk, att0_uv, att0_o, att1_q, att1_uk, att1_uv, att1_o, ffn0_gate, ffn0_up, ffn0_down, ffn1_gate, ffn1_up, ffn1_down, exp_gate, exp_up, exp_down):
        return call_layer(
            kv_lens, hidden_in, route_ids.T, route_wts.T,
            *attention_operands(att0_q, att0_uk, att0_uv, att0_o, cache0),
            *attention_operands(att1_q, att1_uk, att1_uv, att1_o, cache1),
            ffn0_gate.T, ffn0_up.T, ffn0_down, ffn1_gate.T, ffn1_up.T, ffn1_down, exp_gate, exp_up, exp_down)

    return jax.shard_map(body, mesh=mesh, in_specs=in_specs, out_specs=rows_spec, check_vma=False)
```
